128 devices in a mesh: section: 8 (over z, x_lo), dp: 16 (over x_hi, y, core).
Axes of the slice: x: 4 (x_hi: 2, x_lo: 2; x = x_hi * 2 + x_lo), y: 4, z: 4, core: 2. Of those that a mesh axis runs over, the one named last changes fastest.
Arguments:
- acts: bfloat16 [8, 6144, 8192], P('section', 'dp'), may hold values from -6 to 6
- input_grads: bfloat16 [8, 6144, 5120], P('section', 'dp'), may hold values from -6 to 6
- head_grads: bfloat16 [6144, 5120], P('dp'), may hold values from -6 to 6
- weight_grad: bfloat16 [8, 5120, 8192], P('section', None, 'dp'), may hold values from -6 to 6
- sweeps: int32 [8, 52], P('section'), may hold values from 1 to 4
Outputs:
- update: bfloat16 [8, 5120, 8192], P('section', None, 'dp')
The draws below stay inside these ranges and needn't reach their ends.
Inputs may be any that keep to these rules, and one draw needn't show every extreme that they name: sweeps[s, k] is the number of Newton-Schulz iterations of block k of layer s; every value from 1 to 4 occurs.
All inputs are finite; a program needn't handle non-finite values. Where the reference program divides by a largest or mean magnitude, that divisor is 1e-20 or more.
Results may differ from the reference program's by a relative error of at most 0.0067.
Values may be sent and summed in bfloat16 or wider, within the bound.
A program may use at most 128 MiB of HBM per device.

```python
import jax
import jax.numpy as jnp
from jax import lax

D = 5120
H = 8192
BLOCK = 256
NS_MAX = 4
SECTIONS = 8
TOKENS = 6144
NBLK = 52


def with_ends(values, rng, smallest, high):
    longest = values.shape.index(max(values.shape))
    spots = []
    for shift in (0, 1):
        where = [jax.random.randint(jax.random.fold_in(rng, axis), (), 0, length) for axis, length in enumerate(values.shape)]
        where[longest] = (where[longest] + shift) % values.shape[longest]
        spots.append(tuple(where))
    return values.at[spots[0]].set(smallest).at[spots[1]].set(high)


def steps_of(own_key, shape, cuts, low, top_value):
    level = 1.0
    for position, parts in cuts:
        steps = jax.random.uniform(jax.random.fold_in(jax.random.fold_in(own_key, 6), position), (parts,), jnp.float32, low / len(cuts), top_value / len(cuts))
        level = level * jnp.repeat(jnp.exp(steps), shape[position] // parts).reshape((-1,) + (1,) * (len(shape) - 1 - position))
    return level


def centred(rng, shape, deviation, bound, split=(), kind=jnp.bfloat16):
    level = steps_of(rng, shape, split, -0.22, 0.18) if split else 1.0
    drawn = jax.random.normal(rng, shape, jnp.float32) * deviation * level
    return jnp.minimum(jnp.maximum(drawn, -bound), bound).astype(kind)


def setup_inputs(seed: int = 0) -> dict:
    streams_of = jax.random.split(jax.random.key(seed), 6)
    return {
        "acts": centred(streams_of[0], (SECTIONS, TOKENS, H), 1.0, 6.0, ((0, 8), (1, 16))),
        "input_grads": centred(streams_of[1], (SECTIONS, TOKENS, D), 1.0, 6.0, ((0, 8), (1, 16))),
        "head_grads": centred(streams_of[2], (TOKENS, D), 1.0, 6.0, ((0, 16),)),
        "weight_grad": centred(streams_of[3], (SECTIONS, D, H), 1.0, 6.0, ((0, 8), (2, 16))),
        "sweeps": with_ends(jax.random.randint(streams_of[4], (SECTIONS, NBLK), 1, NS_MAX + 1), jax.random.fold_in(streams_of[4], 1), 1, NS_MAX).astype(jnp.int32),
    }


damping = 0.05


def newton_blocks(matrices, counts):
    size = matrices.shape[-1]
    eye = jnp.eye(size, dtype=jnp.float32)
    scale = 1.0 / jnp.max(jnp.sum(jnp.abs(matrices), axis=2), axis=1)
    approx = scale[:, None, None] * eye[None]
    for turn in range(NS_MAX):
        inner = 2.0 * eye[None] - jnp.einsum("kab,kbc->kac", matrices, approx, precision=lax.Precision.HIGHEST)
        fresh = jnp.einsum("kab,kbc->kac", approx, inner, precision=lax.Precision.HIGHEST)
        approx = jnp.where((turn < counts)[:, None, None], fresh, approx)
    return approx


def reference(acts, input_grads, head_grads, weight_grad, sweeps):
    eye = jnp.eye(BLOCK, dtype=jnp.float32)
    hidden_blocks = H // BLOCK
    model_blocks = D // BLOCK
    results = []
    for layer in range(SECTIONS):
        inputs = acts[layer].astype(jnp.float32).reshape(TOKENS, hidden_blocks, BLOCK)
        if layer + 1 < SECTIONS:
            grads = input_grads[layer + 1]
        else:
            grads = head_grads
        grads = grads.astype(jnp.float32).reshape(TOKENS, model_blocks, BLOCK)
        side_a = jnp.einsum("tkb,tkc->kbc", inputs, inputs, precision=lax.Precision.HIGHEST)
        side_g = jnp.einsum("tkb,tkc->kbc", grads, grads, precision=lax.Precision.HIGHEST)
        factors = jnp.concatenate([side_a, side_g], axis=0) / TOKENS + damping * eye[None]
        inverse = newton_blocks(factors, sweeps[layer]).astype(jnp.bfloat16)
        inverse_a = inverse[:hidden_blocks].astype(jnp.float32)
        inverse_g = inverse[hidden_blocks:].astype(jnp.float32)
        weights = weight_grad[layer].astype(jnp.float32).reshape(D, hidden_blocks, BLOCK)
        half = jnp.einsum("dkb,kbc->dkc", weights, inverse_a, precision=lax.Precision.HIGHEST).astype(jnp.bfloat16)
        half = half.reshape(model_blocks, BLOCK, H).astype(jnp.float32)
        update = jnp.einsum("kab,kbc->kac", inverse_g, half, precision=lax.Precision.HIGHEST)
        results.append(update.reshape(D, H).astype(jnp.bfloat16))
    return jnp.stack(results)
```

```python
import functools

import jax
import jax.numpy as jnp
from jax import lax
from jax.experimental import pallas as pl
from jax.experimental.pallas import tpu as pltpu
from jax.sharding import PartitionSpec as P

BLOCK = 256
HALF = 128
ROWS = 272
DAMPING = 0.05
F32 = jnp.float32
BF16 = jnp.bfloat16
MESH = pl.DeviceIdType.MESH


def iotas(rows, columns):
    return (
        lax.broadcasted_iota(jnp.int32, (rows, columns), 0),
        lax.broadcasted_iota(jnp.int32, (rows, columns), 1),
    )


def store_diagonals(dst, i, both):
    high = both.astype(BF16)
    low = both - high.astype(F32)
    dst[i, pl.ds(BLOCK, 16), :] = jnp.concatenate([high.astype(F32), low], axis=0).astype(BF16)


def store_packed(dst, i, full):
    row, column = iotas(HALF, HALF)
    first, off, last = full[:HALF, :HALF], full[:HALF, HALF:], full[HALF:, HALF:]
    dst[i, pl.ds(0, HALF), :] = jnp.where(row <= column, first, last).astype(BF16)
    dst[i, pl.ds(HALF, HALF), :] = off.astype(BF16)
    d_first = jnp.sum(jnp.where(row == column, first, 0.0), axis=0, keepdims=True)
    d_last = jnp.sum(jnp.where(row == column, last, 0.0), axis=0, keepdims=True)
    row8, _ = iotas(8, HALF)
    both = jnp.where(row8 == 0, d_first, jnp.where(row8 == 1, d_last, 0.0))
    store_diagonals(dst, i, both)


def add_packed(dst, di, a, ai, b, bi):
    dst[di, pl.ds(0, BLOCK), :] = (
        a[ai, pl.ds(0, BLOCK), :].astype(F32) + b[bi, pl.ds(0, BLOCK), :].astype(F32)
    ).astype(BF16)
    total = a[ai, pl.ds(BLOCK, 16), :].astype(F32) + b[bi, pl.ds(BLOCK, 16), :].astype(F32)
    store_diagonals(dst, di, total[:8] + total[8:])


def unpack(selected, off, both):
    row, column = iotas(HALF, HALF)
    flipped = selected.T
    first = jnp.where(row == column, both[0:1], jnp.where(row <= column, selected, flipped))
    last = jnp.where(row == column, both[1:2], jnp.where(row > column, selected, flipped))
    return jnp.concatenate(
        [jnp.concatenate([first, off], axis=1), jnp.concatenate([off.T, last], axis=1)], axis=0
    )


def load_full(src, i):
    tail = src[i, pl.ds(BLOCK, 16), :].astype(F32)
    return unpack(
        src[i, pl.ds(0, HALF), :].astype(F32),
        src[i, pl.ds(HALF, HALF), :].astype(F32),
        tail[:8] + tail[8:],
    )


def load_full_sum(a, ai, b, bi):
    both = [
        a[ai, pl.ds(start, size), :].astype(F32) + b[bi, pl.ds(start, size), :].astype(F32)
        for start, size in ((0, HALF), (HALF, HALF), (BLOCK, 16))
    ]
    return unpack(both[0], both[1], both[2][:8] + both[2][8:])


def split(x):
    high = x.astype(BF16)
    return high, (x - high.astype(F32)).astype(BF16)


def product(a, b):
    a_high, a_low = split(a)
    b_high, b_low = split(b)
    left = jnp.concatenate([a_high, a_high, a_low], axis=1)
    right = jnp.concatenate([b_high, b_low, b_high], axis=0)
    return jnp.dot(left, right, preferred_element_type=F32)


def newton(matrix, count):
    row, column = iotas(BLOCK, BLOCK)
    eye = jnp.where(row == column, 1.0, 0.0).astype(F32)
    norm = jnp.max(jnp.sum(jnp.abs(matrix), axis=0, keepdims=True), axis=1, keepdims=True)
    scale = 1.0 / norm
    residual = eye - scale * matrix
    approx = scale * (eye + residual)
    chosen = approx
    residual = product(residual, residual)
    for turn in range(1, 4):
        if turn < 3:
            both = product(jnp.concatenate([residual, approx], axis=0), residual)
            approx = approx + both[BLOCK:]
            residual = both[:BLOCK]
        else:
            approx = approx + product(approx, residual)
        chosen = jnp.where(count > turn, approx, chosen)
    return chosen


def exchange_kernel(
    tokens, sweeps, acts, grads, head, inv_a, inv_g,
    x_a, x_g, gs1, go1, gr1, gs2, go2, gr2, gs3, go3, gr3, gs4, gx0, gx1, x3, r2, y3, y2, dx3, dr2, dy3, dy2,
    as1, ao1, ar1, as2, ao2, ar2, as3, ao3, ar3, as4, ao4, ar4, load_sem, send_sem, recv_sem,
):
    section = lax.axis_index("section")
    dp = lax.axis_index("dp")
    core = lax.rem(dp, 2)
    y = lax.rem(dp // 2, 4)
    x = dp // 8
    y_low, y_high = lax.rem(y, 2), y // 2
    y_odd = lax.rem(y_low + y_high, 2)
    near = y + 1 - 2 * y_low
    far = 3 - y
    first_y = jnp.where(core == 0, near, far)
    second_y = jnp.where(core == 0, far, near)
    b1 = jnp.where(core == 0, y_odd, y_high)
    b2 = jnp.where(core == 0, y_high, y_odd)
    n1, n2 = 1 - b1, 1 - b2
    p_core = (section, dp + 1 - 2 * core)
    p_y1 = (section, x * 8 + first_y * 2 + core)
    p_y2 = (section, x * 8 + second_y * 2 + core)
    p_x = (section, lax.rem(dp + 8, 16))
    below, above = lax.rem(section + 7, 8), lax.rem(section + 1, 8)
    p_straight = (below, dp)
    p_cross = (below, lax.rem(dp + 8, 16))

    def rdma(i, src, dst, target):
        return pltpu.make_async_remote_copy(
            src_ref=src, dst_ref=dst, send_sem=send_sem.at[i], recv_sem=recv_sem.at[i],
            device_id=target, device_id_type=MESH,
        )

    g_chunk, a_chunk = x_g.shape[1] // 2, x_a.shape[1] // 4

    def load_g(i, src):
        part = pl.ds(pl.multiple_of(i * g_chunk, BLOCK), g_chunk)
        return pltpu.make_async_copy(src.at[:, part], x_g.at[:, part], load_sem.at[i])

    def load_a(i):
        part = pl.ds(i * a_chunk, a_chunk)
        return pltpu.make_async_copy(acts.at[0, :, part], x_a.at[:, part], load_sem.at[2 + i])

    g_order = (1 - core, core)

    @pl.when(section == 0)
    def _():
        for i in range(2):
            pltpu.make_async_copy(
                head.at[:, pl.ds(i * g_chunk, g_chunk)], x_g.at[:, pl.ds(i * g_chunk, g_chunk)], load_sem.at[i]
            ).start()

    @pl.when(section > 0)
    def _():
        for i in range(2):
            pltpu.make_async_copy(
                grads.at[0, :, pl.ds(i * g_chunk, g_chunk)], x_g.at[:, pl.ds(i * g_chunk, g_chunk)], load_sem.at[i]
            ).start()

    for i in range(4):
        load_a(i).start()

    barrier = pltpu.get_barrier_semaphore()
    greeted = (p_core, p_y1, p_y2, p_x, p_straight, p_cross, (above, dp), (above, lax.rem(dp + 8, 16)))
    for target in greeted:
        pl.semaphore_signal(barrier, inc=1, device_id=target, device_id_type=MESH)

    def outer(ref, block):
        columns = pl.ds(pl.multiple_of(block * BLOCK, BLOCK), BLOCK)
        tile = ref[:, columns]
        return lax.dot_general(tile, tile, (((0,), (0,)), ((), ())), preferred_element_type=F32)

    def g_partials(dst, which):
        @pl.loop(0, 10)
        def _(i):
            store_packed(dst, i, outer(x_g, which * 10 + i))

    def a_block(q, j):
        q_core = q // 8
        h1, h2, h3 = lax.rem(q // 4, 2), lax.rem(q // 2, 2), lax.rem(q, 2)
        odd = lax.rem(h1 + h2, 2)
        high = jnp.where(q_core == 0, h2, h1)
        low = odd
        owner = h3 * 8 + (high * 2 + low) * 2 + q_core
        return owner * 2 + j

    def a_partials(dst, which, start, stop):
        @pl.loop(start, stop)
        def _(i):
            store_packed(dst, i, outer(x_a, a_block(which * 8 + i // 2, lax.rem(i, 2))))

    def add_blocks(dst, size, a, b, start):
        @pl.loop(0, size)
        def _(i):
            add_packed(dst, i, a, start + i, b, start + i)

    load_g(0, head).wait()
    load_g(1, head).wait()
    g_partials(gs1, 1 - core)
    pl.semaphore_wait(barrier, len(greeted))
    g_core = rdma(0, gs1, gr1, p_core)
    g_core.start()
    g_partials(go1, core)
    g_core.wait()
    add_blocks(gs2, 5, go1, gr1, n1 * 5)
    g_y1 = rdma(1, gs2, gr2, p_y1)
    g_y1.start()
    add_blocks(go2, 5, go1, gr1, b1 * 5)
    for i in range(4):
        load_a(i).wait()
    a_partials(as1, 1 - core, 0, 16)
    a_core = rdma(9, as1, ar1, p_core)
    a_core.start()
    a_partials(ao1, core, 0, 4)
    g_y1.wait()
    add_blocks(gs3, 3, go2, gr2, n2 * 2)
    g_y2 = rdma(2, gs3, gr3, p_y2)
    g_y2.start()
    add_blocks(go3, 3, go2, gr2, b2 * 2)
    a_partials(ao1, core, 4, 16)
    g_y2.wait()
    g_over = []
    for i in range(3):
        add_packed(gs4, i, go3, i, gr3, i)
        for base, dst, target in ((3, gx0, p_straight), (6, gx1, p_cross)):
            copy = rdma(base + i, gs4.at[i], dst.at[i], target)
            copy.start()
            g_over.append(copy)
    a_core.wait()
    add_blocks(as2, 8, ao1, ar1, n1 * 8)
    a_y1 = rdma(10, as2, ar2, p_y1)
    a_y1.start()
    add_blocks(ao2, 8, ao1, ar1, b1 * 8)
    a_y1.wait()
    add_blocks(as3, 4, ao2, ar2, n2 * 4)
    a_y2 = rdma(11, as3, ar3, p_y2)
    a_y2.start()
    add_blocks(ao3, 4, ao2, ar2, b2 * 4)

    row, column = iotas(BLOCK, BLOCK)
    damp = jnp.where(row == column, DAMPING, 0.0).astype(F32)
    hidden_blocks = x_a.shape[1] // BLOCK
    g_first = core * 10 + b1 * 5 + b2 * 2
    for i in range(3):
        g_over[2 * i].wait()
        g_over[2 * i + 1].wait()
        factor = load_full_sum(gx0, i, gx1, i) * (1.0 / tokens) + damp
        inverse = newton(factor, sweeps[0, hidden_blocks + g_first + i])
        store_packed(x3, i, inverse)
    x3_y1 = rdma(14, x3, y3, p_y1)
    x3_y2 = rdma(13, x3.at[pl.ds(b2, 2)], r2, p_y2)
    x3_core = rdma(16, x3, dx3, p_core)
    x3_y2.start()
    x3_y1.start()
    x3_core.start()

    def expand(src, size, start):
        @pl.loop(0, size)
        def _(i):
            inv_g[start + i, :, :] = load_full(src, i).astype(BF16)

    a_y2.wait()
    add_blocks(as4, 2, ao3, ar3, (1 - x) * 2)
    a_x = rdma(12, as4, ar4, p_x)
    a_x.start()
    add_blocks(ao4, 2, ao3, ar3, x * 2)
    expand(x3, 3, g_first)
    x3_y2.wait()
    r2_y1 = rdma(15, r2, y2, p_y1)
    r2_core = rdma(17, r2, dr2, p_core)
    r2_y1.start()
    r2_core.start()
    expand(r2, 2, core * 10 + b1 * 5 + n2 * 3)
    x3_y1.wait()
    y3_core = rdma(18, y3, dy3, p_core)
    y3_core.start()
    expand(y3, 3, core * 10 + n1 * 5 + b2 * 2)
    r2_y1.wait()
    y2_core = rdma(19, y2, dy2, p_core)
    y2_core.start()
    expand(y2, 2, core * 10 + n1 * 5 + n2 * 3)
    other = (1 - core) * 10
    x3_core.wait()
    expand(dx3, 3, other + b2 * 5 + b1 * 2)
    r2_core.wait()
    expand(dr2, 2, other + b2 * 5 + n1 * 3)
    a_x.wait()
    for j in range(2):
        factor = load_full_sum(ao4, j, ar4, j) * (1.0 / tokens) + damp
        inv_a[j, :, :] = newton(factor, sweeps[0, dp * 2 + j]).astype(BF16)
    y3_core.wait()
    expand(dy3, 3, other + n2 * 5 + b1 * 2)
    y2_core.wait()
    expand(dy2, 2, other + n2 * 5 + n1 * 3)


def packed(count):
    return pltpu.VMEM((count, ROWS, HALF), BF16)


def exchange(tokens, sweeps, acts, grads, head):
    hbm = pl.BlockSpec(memory_space=pl.ANY)
    vmem = pl.BlockSpec(memory_space=pltpu.VMEM)
    rows = acts.shape[1]
    model_blocks = grads.shape[2] // BLOCK
    counts = (10, 10, 10, 5, 5, 5, 3, 3, 3, 3, 3, 3, 3, 2, 3, 2, 3, 2, 3, 2)
    a_counts = (16, 16, 16, 8, 8, 8, 4, 4, 4, 2, 2, 2)
    return pl.pallas_call(
        functools.partial(exchange_kernel, tokens),
        out_shape=(
            jax.ShapeDtypeStruct((2, BLOCK, BLOCK), BF16),
            jax.ShapeDtypeStruct((model_blocks, BLOCK, BLOCK), BF16),
        ),
        in_specs=[pl.BlockSpec(memory_space=pltpu.SMEM), hbm, hbm, hbm],
        out_specs=(vmem, vmem),
        scratch_shapes=[
            pltpu.VMEM((rows, acts.shape[2]), BF16),
            pltpu.VMEM((rows, grads.shape[2]), BF16),
            *[packed(n) for n in counts],
            *[packed(n) for n in a_counts],
            pltpu.SemaphoreType.DMA((6,)),
            pltpu.SemaphoreType.DMA((20,)),
            pltpu.SemaphoreType.DMA((20,)),
        ],
        compiler_params=pltpu.CompilerParams(
            collective_id=0, has_side_effects=True, vmem_limit_bytes=60 * 1024 * 1024
        ),
        name="exchange",
    )(sweeps, acts, grads, head)


def apply_kernel(weights, inv_a, inv_g, out):
    halves = [
        jnp.dot(weights[0, :, j * BLOCK : (j + 1) * BLOCK], inv_a[j], preferred_element_type=F32).astype(BF16)
        for j in range(2)
    ]
    half = jnp.concatenate(halves, axis=1)
    out[0, :, :] = jnp.dot(inv_g[0], half, preferred_element_type=F32).astype(BF16)


def apply(weights, inv_a, inv_g):
    _, rows, columns = weights.shape
    return pl.pallas_call(
        apply_kernel,
        out_shape=jax.ShapeDtypeStruct(weights.shape, BF16),
        grid=(rows // BLOCK,),
        in_specs=[
            pl.BlockSpec((1, BLOCK, columns), lambda k: (0, k, 0)),
            pl.BlockSpec((2, BLOCK, BLOCK), lambda k: (0, 0, 0)),
            pl.BlockSpec((1, BLOCK, BLOCK), lambda k: (k, 0, 0)),
        ],
        out_specs=pl.BlockSpec((1, BLOCK, columns), lambda k: (0, k, 0)),
        name="apply",
    )(weights, inv_a, inv_g)


def on_device(acts, input_grads, head_grads, weight_grad, sweeps):
    tokens = acts.shape[1] * lax.axis_size("dp")
    inv_a, inv_g = exchange(tokens, sweeps, acts, input_grads, head_grads)
    return apply(weight_grad, inv_a, inv_g)


def solution(mesh):
    return jax.shard_map(
        on_device,
        mesh=mesh,
        in_specs=(
            P("section", "dp", None),
            P("section", "dp", None),
            P("dp", None),
            P("section", None, "dp"),
            P("section", None),
        ),
        out_specs=P("section", None, "dp"),
        check_vma=False,
    )
```

```python
import functools

import jax
import jax.numpy as jnp
from jax import lax
from jax.experimental import pallas as pl
from jax.experimental.pallas import tpu as pltpu
from jax.sharding import PartitionSpec as P

BLOCK = 256
HALF = 128
ROWS = 272
DAMPING = 0.05
F32 = jnp.float32
BF16 = jnp.bfloat16
MESH = pl.DeviceIdType.MESH


def iotas(rows, columns):
    return (
        lax.broadcasted_iota(jnp.int32, (rows, columns), 0),
        lax.broadcasted_iota(jnp.int32, (rows, columns), 1),
    )


def store_diagonals(dst, i, both):
    high = both.astype(BF16)
    low = both - high.astype(F32)
    dst[i, pl.ds(BLOCK, 16), :] = jnp.concatenate([high.astype(F32), low], axis=0).astype(BF16)


def store_packed(dst, i, full):
    row, column = iotas(HALF, HALF)
    first, off, last = full[:HALF, :HALF], full[:HALF, HALF:], full[HALF:, HALF:]
    dst[i, pl.ds(0, HALF), :] = jnp.where(row <= column, first, last).astype(BF16)
    dst[i, pl.ds(HALF, HALF), :] = off.astype(BF16)
    d_first = jnp.sum(jnp.where(row == column, first, 0.0), axis=0, keepdims=True)
    d_last = jnp.sum(jnp.where(row == column, last, 0.0), axis=0, keepdims=True)
    row8, _ = iotas(8, HALF)
    both = jnp.where(row8 == 0, d_first, jnp.where(row8 == 1, d_last, 0.0))
    store_diagonals(dst, i, both)


def add_packed(dst, di, a, ai, b, bi):
    dst[di, pl.ds(0, BLOCK), :] = (
        a[ai, pl.ds(0, BLOCK), :].astype(F32) + b[bi, pl.ds(0, BLOCK), :].astype(F32)
    ).astype(BF16)
    total = a[ai, pl.ds(BLOCK, 16), :].astype(F32) + b[bi, pl.ds(BLOCK, 16), :].astype(F32)
    store_diagonals(dst, di, total[:8] + total[8:])


def unpack(selected, off, both):
    row, column = iotas(HALF, HALF)
    flipped = selected.T
    first = jnp.where(row == column, both[0:1], jnp.where(row <= column, selected, flipped))
    last = jnp.where(row == column, both[1:2], jnp.where(row > column, selected, flipped))
    return jnp.concatenate(
        [jnp.concatenate([first, off], axis=1), jnp.concatenate([off.T, last], axis=1)], axis=0
    )


def load_full(src, i):
    tail = src[i, pl.ds(BLOCK, 16), :].astype(F32)
    return unpack(
        src[i, pl.ds(0, HALF), :].astype(F32),
        src[i, pl.ds(HALF, HALF), :].astype(F32),
        tail[:8] + tail[8:],
    )


def load_full_sum(a, ai, b, bi):
    both = [
        a[ai, pl.ds(start, size), :].astype(F32) + b[bi, pl.ds(start, size), :].astype(F32)
        for start, size in ((0, HALF), (HALF, HALF), (BLOCK, 16))
    ]
    return unpack(both[0], both[1], both[2][:8] + both[2][8:])


def split(x):
    high = x.astype(BF16)
    return high, (x - high.astype(F32)).astype(BF16)


def product(a, b):
    a_high, a_low = split(a)
    b_high, b_low = split(b)
    left = jnp.concatenate([a_high, a_high, a_low], axis=1)
    right = jnp.concatenate([b_high, b_low, b_high], axis=0)
    return jnp.dot(left, right, preferred_element_type=F32)


def newton(matrices, counts):
    row, column = iotas(BLOCK, BLOCK)
    eye = jnp.where(row == column, 1.0, 0.0).astype(F32)
    state = []
    for matrix in matrices:
        norm = jnp.max(jnp.sum(jnp.abs(matrix), axis=0, keepdims=True), axis=1, keepdims=True)
        scale = 1.0 / norm
        residual = eye - scale * matrix
        approx = scale * (eye + residual)
        state.append((approx, residual))
    chosen = [approx for approx, _ in state]
    state = [(approx, product(residual, residual)) for approx, residual in state]
    for turn in range(1, 4):
        if turn < 3:
            both = [product(jnp.concatenate([residual, approx], axis=0), residual) for approx, residual in state]
            state = [(approx + b[BLOCK:], b[:BLOCK]) for (approx, _), b in zip(state, both)]
        else:
            state = [(approx + product(approx, residual), None) for approx, residual in state]
        chosen = [jnp.where(count > turn, now, old) for count, (now, _), old in zip(counts, state, chosen)]
    return chosen


def exchange_kernel(
    tokens, sweeps_hbm, acts, grads, head, weights, out, sweeps,
    x_a, x_g, w, half, gs1, go1, gr1, gs2, gr2, gs3, gr3, gs4, gx0, gx1,
    own, r2, y3, y2, d_own, d_r2, d_y3, d_y2,
    as1, ao1, ar1, as2, ar2, as3, ar3, as4, ar4, inv_a, load_sem, send_sem, recv_sem,
):
    section = lax.axis_index("section")
    dp = lax.axis_index("dp")
    core = lax.rem(dp, 2)
    y = lax.rem(dp // 2, 4)
    x = dp // 8
    y_low, y_high = lax.rem(y, 2), y // 2
    y_odd = lax.rem(y_low + y_high, 2)
    near = y + 1 - 2 * y_low
    far = 3 - y
    first_y = jnp.where(core == 0, near, far)
    second_y = jnp.where(core == 0, far, near)
    b1 = jnp.where(core == 0, y_odd, y_high)
    b2 = jnp.where(core == 0, y_high, y_odd)
    n1, n2 = 1 - b1, 1 - b2
    crossed = lax.rem(dp + 8, 16)
    below, above = lax.rem(section + 7, 8), lax.rem(section + 1, 8)
    p_core = (section, dp + 1 - 2 * core)
    p_y1 = (section, x * 8 + first_y * 2 + core)
    p_y2 = (section, x * 8 + second_y * 2 + core)
    p_x = (section, crossed)
    p_straight = (below, dp)
    p_cross = (below, crossed)
    used = []

    def send(src, dst, target):
        i = len(used)
        used.append(i)
        copy = pltpu.make_async_remote_copy(
            src_ref=src, dst_ref=dst, send_sem=send_sem.at[i], recv_sem=recv_sem.at[i],
            device_id=target, device_id_type=MESH,
        )
        copy.start()
        return copy

    g_chunk, a_chunk, w_chunk = x_g.shape[1] // 2, x_a.shape[1] // 2, w.shape[0] // 2
    model_blocks, hidden_blocks = x_g.shape[1] // BLOCK, x_a.shape[1] // BLOCK

    def load_g(i, src):
        part = pl.ds(i * g_chunk, g_chunk)
        return pltpu.make_async_copy(src.at[:, part], x_g.at[:, part], load_sem.at[i])

    def load_a(i):
        part = pl.ds(i * a_chunk, a_chunk)
        return pltpu.make_async_copy(acts.at[0, :, part], x_a.at[:, part], load_sem.at[2 + i])

    def load_w(i):
        part = pl.ds(i * w_chunk, w_chunk)
        return pltpu.make_async_copy(weights.at[0, part, :], w.at[part, :], load_sem.at[4 + i])

    @pl.when(section == 0)
    def _():
        for i in range(2):
            load_g(i, head).start()

    @pl.when(section > 0)
    def _():
        for i in range(2):
            load_g(i, grads.at[0]).start()

    load_sweeps = pltpu.make_async_copy(sweeps_hbm, sweeps, load_sem.at[6])
    load_sweeps.start()
    barrier = pltpu.get_barrier_semaphore()
    greeted = (p_core, p_y1, p_y2, p_x, p_straight, p_cross, (above, dp), (above, crossed))
    for target in greeted:
        pl.semaphore_signal(barrier, inc=1, device_id=target, device_id_type=MESH)

    def outer(ref, block):
        columns = pl.ds(pl.multiple_of(block * BLOCK, BLOCK), BLOCK)
        tile = ref[:, columns]
        return lax.dot_general(tile, tile, (((0,), (0,)), ((), ())), preferred_element_type=F32)

    def place(k, bit):
        return (1 - bit) * 3 + k if k < 2 else 2 if k == 2 else bit * 3 + k - 3

    def g_partials(dst, at, group, bit):
        for k in range(5):
            store_packed(dst, at + k, outer(x_g, group * 5 + place(k, bit)))

    def a_partials(dst, at, of_core, first, second):
        @pl.loop(0, 2)
        def _(e):
            bit = jnp.where(e == 0, 1 - second, second)
            for u in range(2):
                owner = (1 - x if u == 0 else x) * 8
                for j in range(2):
                    for_core_0 = owner + (bit * 2 + lax.rem(first + bit, 2)) * 2
                    for_core_1 = owner + (first * 2 + lax.rem(first + bit, 2)) * 2 + 1
                    block = jnp.where(of_core == 0, for_core_0, for_core_1) * 2 + j
                    store_packed(dst, at + 4 * e + 2 * u + j, outer(x_a, block))

    def add_blocks(dst, di, size, a, ai, b, bi):
        @pl.loop(0, size)
        def _(i):
            add_packed(dst, di + i, a, ai + i, b, bi + i)

    load_g(0, head).wait()
    load_g(1, head).wait()
    for i in range(2):
        load_a(i).start()
    o_core = 1 - core
    g_partials(gs1, 0, o_core * 2 + n2, b1)
    pl.semaphore_wait(barrier, len(greeted))
    g_core = [send(gs1.at[pl.ds(0, 5)], gr1.at[pl.ds(0, 5)], p_core)]
    g_partials(go1, 0, core * 2 + n1, b2)
    g_core[0].wait()
    g_y1 = []
    for k in range(5):
        add_packed(gs2, k, go1, k, gr1, k)
        g_y1.append(send(gs2.at[k], gr2.at[k], p_y1))
    g_partials(gs1, 5, o_core * 2 + b2, b1)
    g_core.append(send(gs1.at[pl.ds(5, 5)], gr1.at[pl.ds(5, 5)], p_core))
    g_partials(go1, 5, core * 2 + b1, b2)
    for i in range(2):
        load_a(i).wait()
    for i in range(2):
        load_w(i).start()
    a_partials(as1, 0, o_core, n2, b1)
    a_core = [send(as1.at[pl.ds(0, 8)], ar1.at[pl.ds(0, 8)], p_core)]
    a_partials(ao1, 0, core, n1, b2)
    g_core[1].wait()
    add_blocks(go1, 5, 5, go1, 5, gr1, 5)
    g_y2 = []
    for k in range(3):
        g_y1[k].wait()
        add_packed(gs3, k, go1, 5 + k, gr2, k)
        g_y2.append(send(gs3.at[k], gr3.at[k], p_y2))
    a_core[0].wait()
    a_y1 = []
    for i in range(2):
        add_blocks(as2, 4 * i, 4, ao1, 4 * i, ar1, 4 * i)
        a_y1.append(send(as2.at[pl.ds(4 * i, 4)], ar2.at[pl.ds(4 * i, 4)], p_y1))
    a_partials(as1, 8, o_core, b2, b1)
    a_core.append(send(as1.at[pl.ds(8, 8)], ar1.at[pl.ds(8, 8)], p_core))
    g_over = []
    for k in range(3):
        mine = (8, 9, 7)[k]
        g_y2[k].wait()
        if k < 2:
            g_y1[3 + k].wait()
        add_packed(go1, mine, go1, mine, gr2, mine - 5)
        add_packed(gs4, k, go1, mine, gr3, k)
        g_over.append((send(gs4.at[k], gx0.at[k], p_straight), send(gs4.at[k], gx1.at[k], p_cross)))
    a_partials(ao1, 8, core, b1, b2)
    a_core[1].wait()
    add_blocks(ao1, 8, 8, ao1, 8, ar1, 8)
    a_y1[0].wait()
    add_blocks(as3, 0, 4, ao1, 8, ar2, 0)
    a_y2 = [send(as3.at[pl.ds(2 * i, 2)], ar3.at[pl.ds(2 * i, 2)], p_y2) for i in range(2)]
    a_y1[1].wait()
    add_blocks(ao1, 12, 4, ao1, 12, ar2, 4)
    load_sweeps.wait()
    row, column = iotas(BLOCK, BLOCK)
    damp = jnp.where(row == column, DAMPING, 0.0).astype(F32)
    mean = 1.0 / tokens
    here, there = core * 10, o_core * 10
    g_own, g_r2, g_own_core, g_y3_core = [], [], [], []

    def g_invert(k):
        g_over[k][0].wait()
        g_over[k][1].wait()
        factor = load_full_sum(gx0, k, gx1, k) * mean + damp
        at = here + b1 * 5 + (b2 * 3 + k if k < 2 else 2)
        store_packed(own, k, newton([factor], [sweeps[0, hidden_blocks + at]])[0])
        if k < 2:
            g_r2.append(send(own.at[k], r2.at[k], p_y2))
        g_own.append(send(own.at[k], y3.at[k], p_y1))
        g_own_core.append(send(own.at[k], d_own.at[k], p_core))

    g_invert(0)
    a_y2[0].wait()
    add_blocks(as4, 0, 2, ao1, 12, ar3, 0)
    a_x = send(as4, ar4, p_x)
    a_y2[1].wait()
    add_blocks(ao1, 14, 2, ao1, 14, ar3, 2)
    g_invert(1)
    g_invert(2)
    for i in range(2):
        load_w(i).wait()
    relayed, y2_core = [], []

    def relay(k):
        g_r2[k].wait()
        relayed.append((send(r2.at[k], y2.at[k], p_y1), send(r2.at[k], d_r2.at[k], p_core)))

    def pass_own(k):
        g_own[k].wait()
        g_y3_core.append(send(y3.at[k], d_y3.at[k], p_core))

    def pass_y2(k):
        relayed[k][0].wait()
        y2_core.append(send(y2.at[k], d_y2.at[k], p_core))

    relay(0)
    relay(1)
    a_x.wait()
    factors = [load_full_sum(ao1, 14 + j, ar4, j) * mean + damp for j in range(2)]
    for j, inverse in enumerate(newton(factors, [sweeps[0, dp * 2 + j] for j in range(2)])):
        inv_a[j, :, :] = inverse.astype(BF16)
    for k in range(3):
        pass_own(k)

    def halves(start, stop):
        @pl.loop(start // 2, stop // 2)
        def _(k):
            rows = pl.ds(pl.multiple_of(k * 2 * BLOCK, 2 * BLOCK), 2 * BLOCK)
            for j in range(2):
                columns = slice(j * BLOCK, (j + 1) * BLOCK)
                half[rows, columns] = jnp.dot(w[rows, columns], inv_a[j], preferred_element_type=F32).astype(BF16)

    halves(0, 10)
    pass_y2(0)
    pass_y2(1)
    halves(10, model_blocks)

    def apply(src, i, block):
        rows = pl.ds(pl.multiple_of(block * BLOCK, BLOCK), BLOCK)
        inverse = load_full(src, i).astype(BF16)
        out[0, rows, :] = jnp.dot(inverse, half[rows, :], preferred_element_type=F32).astype(BF16)

    def apply_own(src, group, bit):
        for k in range(3):
            apply(src, k, group + (bit * 3 + k if k < 2 else 2))

    def apply_r2(src, group, bit):
        for k in range(2):
            apply(src, k, group + bit * 3 + k)

    apply_own(own, here + b1 * 5, b2)
    apply_r2(r2, here + b1 * 5, n2)
    apply_own(y3, here + n1 * 5, b2)
    apply_r2(y2, here + n1 * 5, n2)
    for k in range(3):
        g_own_core[k].wait()
    apply_own(d_own, there + b2 * 5, b1)
    for k in range(2):
        relayed[k][1].wait()
    apply_r2(d_r2, there + b2 * 5, n1)
    for k in range(3):
        g_y3_core[k].wait()
    apply_own(d_y3, there + n2 * 5, b1)
    for k in range(2):
        y2_core[k].wait()
    apply_r2(d_y2, there + n2 * 5, n1)


def packed(count):
    return pltpu.VMEM((count, ROWS, HALF), BF16)


def exchange(tokens, sweeps, acts, grads, head, weights):
    hbm = pl.BlockSpec(memory_space=pltpu.HBM)
    vmem = pl.BlockSpec(memory_space=pltpu.VMEM)
    operands = [pltpu.with_memory_space_constraint(a, pltpu.HBM) for a in (sweeps, acts, grads, head, weights)]
    rows = acts.shape[1]
    g_counts = (10, 10, 10, 5, 5, 3, 3, 3, 3, 3)
    gather_counts = (3, 2, 3, 2, 3, 2, 3, 2)
    a_counts = (16, 16, 16, 8, 8, 4, 4, 2, 2)
    return pl.pallas_call(
        functools.partial(exchange_kernel, tokens),
        out_shape=pltpu.VMEM(weights.shape, BF16),
        in_specs=[hbm] * 5,
        out_specs=vmem,
        scratch_shapes=[
            pltpu.SMEM(sweeps.shape, jnp.int32),
            pltpu.VMEM((rows, acts.shape[2]), BF16),
            pltpu.VMEM((rows, grads.shape[2]), BF16),
            pltpu.VMEM(weights.shape[1:], BF16),
            pltpu.VMEM(weights.shape[1:], BF16),
            *[packed(n) for n in g_counts + gather_counts + a_counts],
            pltpu.VMEM((2, BLOCK, BLOCK), BF16),
            pltpu.SemaphoreType.DMA((7,)),
            pltpu.SemaphoreType.DMA((41,)),
            pltpu.SemaphoreType.DMA((41,)),
        ],
        compiler_params=pltpu.CompilerParams(
            collective_id=0, has_side_effects=True, vmem_limit_bytes=44 * 1024 * 1024
        ),
        name="exchange",
    )(*operands)


def store_kernel(src, dst, sem):
    copy = pltpu.make_async_copy(src, dst, sem)
    copy.start()
    copy.wait()


def store(update):
    return pl.pallas_call(
        store_kernel,
        out_shape=jax.ShapeDtypeStruct(update.shape, update.dtype),
        in_specs=[pl.BlockSpec(memory_space=pltpu.VMEM)],
        out_specs=pl.BlockSpec(memory_space=pltpu.HBM),
        scratch_shapes=[pltpu.SemaphoreType.DMA],
        compiler_params=pltpu.CompilerParams(vmem_limit_bytes=1024 * 1024),
        name="store",
    )(update)


def on_device(acts, input_grads, head_grads, weight_grad, sweeps):
    tokens = acts.shape[1] * lax.axis_size("dp")
    return store(exchange(tokens, sweeps, acts, input_grads, head_grads, weight_grad))


def solution(mesh):
    return jax.shard_map(
        on_device,
        mesh=mesh,
        in_specs=(
            P("section", "dp", None),
            P("section", "dp", None),
            P("dp", None),
            P("section", None, "dp"),
            P("section", None),
        ),
        out_specs=P("section", None, "dp"),
        check_vma=False,
    )
```

```python
import functools

import jax
import jax.numpy as jnp
from jax import lax
from jax.experimental import pallas as pl
from jax.experimental.pallas import tpu as pltpu
from jax.sharding import PartitionSpec as P

BLOCK = 256
HALF = 128
ROWS = 272
DAMPING = 0.05
F32 = jnp.float32
BF16 = jnp.bfloat16
MESH = pl.DeviceIdType.MESH


def iotas(rows, columns):
    return (
        lax.broadcasted_iota(jnp.int32, (rows, columns), 0),
        lax.broadcasted_iota(jnp.int32, (rows, columns), 1),
    )


def store_diagonals(dst, i, both):
    high = both.astype(BF16)
    low = both - high.astype(F32)
    dst[i, pl.ds(BLOCK, 16), :] = jnp.concatenate([high.astype(F32), low], axis=0).astype(BF16)


def store_packed(dst, i, full):
    row, column = iotas(HALF, HALF)
    first, off, last = full[:HALF, :HALF], full[:HALF, HALF:], full[HALF:, HALF:]
    dst[i, pl.ds(0, HALF), :] = jnp.where(row <= column, first, last).astype(BF16)
    dst[i, pl.ds(HALF, HALF), :] = off.astype(BF16)
    d_first = jnp.sum(jnp.where(row == column, first, 0.0), axis=0, keepdims=True)
    d_last = jnp.sum(jnp.where(row == column, last, 0.0), axis=0, keepdims=True)
    row8, _ = iotas(8, HALF)
    both = jnp.where(row8 == 0, d_first, jnp.where(row8 == 1, d_last, 0.0))
    store_diagonals(dst, i, both)


def add_packed(dst, di, a, ai, b, bi):
    dst[di, pl.ds(0, BLOCK), :] = (
        a[ai, pl.ds(0, BLOCK), :].astype(F32) + b[bi, pl.ds(0, BLOCK), :].astype(F32)
    ).astype(BF16)
    total = a[ai, pl.ds(BLOCK, 16), :].astype(F32) + b[bi, pl.ds(BLOCK, 16), :].astype(F32)
    store_diagonals(dst, di, total[:8] + total[8:])


def unpack(selected, off, both):
    row, column = iotas(HALF, HALF)
    flipped = selected.T
    first = jnp.where(row == column, both[0:1], jnp.where(row <= column, selected, flipped))
    last = jnp.where(row == column, both[1:2], jnp.where(row > column, selected, flipped))
    return jnp.concatenate(
        [jnp.concatenate([first, off], axis=1), jnp.concatenate([off.T, last], axis=1)], axis=0
    )


def load_full(src, i):
    tail = src[i, pl.ds(BLOCK, 16), :].astype(F32)
    return unpack(
        src[i, pl.ds(0, HALF), :].astype(F32),
        src[i, pl.ds(HALF, HALF), :].astype(F32),
        tail[:8] + tail[8:],
    )


def load_full_sum(a, ai, b, bi):
    both = [
        a[ai, pl.ds(start, size), :].astype(F32) + b[bi, pl.ds(start, size), :].astype(F32)
        for start, size in ((0, HALF), (HALF, HALF), (BLOCK, 16))
    ]
    return unpack(both[0], both[1], both[2][:8] + both[2][8:])


def split(x):
    high = x.astype(BF16)
    return high, (x - high.astype(F32)).astype(BF16)


def product(a, b):
    a_high, a_low = split(a)
    b_high, b_low = split(b)
    left = jnp.concatenate([a_high, a_high, a_low], axis=1)
    right = jnp.concatenate([b_high, b_low, b_high], axis=0)
    return jnp.dot(left, right, preferred_element_type=F32)


def newton(matrices, counts):
    row, column = iotas(BLOCK, BLOCK)
    eye = jnp.where(row == column, 1.0, 0.0).astype(F32)
    state = []
    for matrix in matrices:
        norm = jnp.max(jnp.sum(jnp.abs(matrix), axis=0, keepdims=True), axis=1, keepdims=True)
        scale = 1.0 / norm
        residual = eye - scale * matrix
        approx = scale * (eye + residual)
        state.append((approx, residual))
    chosen = [approx for approx, _ in state]
    state = [(approx, product(residual, residual)) for approx, residual in state]
    for turn in range(1, 4):
        if turn < 3:
            both = [product(jnp.concatenate([residual, approx], axis=0), residual) for approx, residual in state]
            state = [(approx + b[BLOCK:], b[:BLOCK]) for (approx, _), b in zip(state, both)]
        else:
            state = [(approx + product(approx, residual), None) for approx, residual in state]
        chosen = [jnp.where(count > turn, now, old) for count, (now, _), old in zip(counts, state, chosen)]
    return chosen


def exchange_kernel(
    tokens, sweeps_hbm, acts, grads, head, weights, applied, inv_a, sweeps,
    x_a, x_g, w, gs1, go1, gr1, gs2, gr2, gs3, gr3, gs4, gx0, gx1,
    own, r2, y3, y2, d_own, d_r2, d_y3, d_y2,
    as1, ao1, ar1, as2, ar2, as3, ar3, as4, ar4, load_sem, send_sem, recv_sem,
):
    section = lax.axis_index("section")
    dp = lax.axis_index("dp")
    core = lax.rem(dp, 2)
    y = lax.rem(dp // 2, 4)
    x = dp // 8
    y_low, y_high = lax.rem(y, 2), y // 2
    y_odd = lax.rem(y_low + y_high, 2)
    near = y + 1 - 2 * y_low
    far = 3 - y
    first_y = jnp.where(core == 0, near, far)
    second_y = jnp.where(core == 0, far, near)
    b1 = jnp.where(core == 0, y_odd, y_high)
    b2 = jnp.where(core == 0, y_high, y_odd)
    n1, n2 = 1 - b1, 1 - b2
    crossed = lax.rem(dp + 8, 16)
    below, above = lax.rem(section + 7, 8), lax.rem(section + 1, 8)
    p_core = (section, dp + 1 - 2 * core)
    p_y1 = (section, x * 8 + first_y * 2 + core)
    p_y2 = (section, x * 8 + second_y * 2 + core)
    p_x = (section, crossed)
    p_straight = (below, dp)
    p_cross = (below, crossed)
    used = []

    def send(src, dst, target):
        i = len(used)
        used.append(i)
        copy = pltpu.make_async_remote_copy(
            src_ref=src, dst_ref=dst, send_sem=send_sem.at[i], recv_sem=recv_sem.at[i],
            device_id=target, device_id_type=MESH,
        )
        copy.start()
        return copy

    w_chunk = w.shape[0] // 2
    hidden_blocks = x_a.shape[1] // BLOCK
    o_core = 1 - core
    g_groups = (o_core * 2 + n2, core * 2 + n1, o_core * 2 + b2, core * 2 + b1)
    a_groups = ((o_core, n2, b1), (core, n1, b2), (o_core, b2, b1), (core, b1, b2))

    def load_g(i, src):
        part = pl.ds(pl.multiple_of(g_groups[i] * 5 * BLOCK, BLOCK), 5 * BLOCK)
        return pltpu.make_async_copy(src.at[:, part], x_g.at[:, part], load_sem.at[i])

    def leaf(of_core, first, bit, u):
        middle = lax.rem(first + bit, 2)
        return (1 - x if u == 0 else x) * 8 + (jnp.where(of_core == 0, bit, first) * 2 + middle) * 2 + of_core

    def load_a(i, b, u):
        of_core, first, second = a_groups[i]
        owner = leaf(of_core, first, second if b else 1 - second, u)
        part = pl.ds(pl.multiple_of(owner * 2 * BLOCK, 2 * BLOCK), 2 * BLOCK)
        return pltpu.make_async_copy(acts.at[0, :, part], x_a.at[:, part], load_sem.at[4 + i * 4 + b * 2 + u])

    a_loads = [(b, u) for b in range(2) for u in range(2)]

    def load_w(i):
        part = pl.ds(i * w_chunk, w_chunk)
        return pltpu.make_async_copy(weights.at[0, part, :], w.at[part, :], load_sem.at[20 + i])

    @pl.when(section == 0)
    def _():
        for i in range(4):
            load_g(i, head).start()

    @pl.when(section > 0)
    def _():
        for i in range(4):
            load_g(i, grads.at[0]).start()

    load_sweeps = pltpu.make_async_copy(sweeps_hbm, sweeps, load_sem.at[22])
    load_sweeps.start()
    barrier = pltpu.get_barrier_semaphore()
    greeted = (p_core, p_y1, p_y2, p_x, p_straight, p_cross, (above, dp), (above, crossed))
    for target in greeted:
        pl.semaphore_signal(barrier, inc=1, device_id=target, device_id_type=MESH)

    def outer(ref, block):
        columns = pl.ds(pl.multiple_of(block * BLOCK, BLOCK), BLOCK)
        tile = ref[:, columns]
        return lax.dot_general(tile, tile, (((0,), (0,)), ((), ())), preferred_element_type=F32)

    def place(k, bit):
        return (1 - bit) * 3 + k if k < 2 else 2 if k == 2 else bit * 3 + k - 3

    def g_partials(dst, at, i):
        load_g(i, head).wait()
        bit = (b1, b2)[i % 2]
        for k in range(5):
            store_packed(dst, at + k, outer(x_g, g_groups[i] * 5 + place(k, bit)))

    def a_partials(dst, at, i):
        of_core, first, second = a_groups[i]
        for b, u in a_loads:
            load_a(i, b, u).wait()

        @pl.loop(0, 2)
        def _(e):
            bit = jnp.where(e == 0, 1 - second, second)
            for u in range(2):
                owner = leaf(of_core, first, bit, u)
                for j in range(2):
                    store_packed(dst, at + 4 * e + 2 * u + j, outer(x_a, owner * 2 + j))

    def add_blocks(dst, di, size, a, ai, b, bi):
        @pl.loop(0, size)
        def _(i):
            add_packed(dst, di + i, a, ai + i, b, bi + i)

    g_partials(gs1, 0, 0)
    for i in range(4):
        for b, u in a_loads:
            load_a(i, b, u).start()
    pl.semaphore_wait(barrier, len(greeted))
    g_core = [send(gs1.at[pl.ds(0, 5)], gr1.at[pl.ds(0, 5)], p_core)]
    g_partials(go1, 0, 1)
    g_partials(gs1, 5, 2)
    g_core.append(send(gs1.at[pl.ds(5, 5)], gr1.at[pl.ds(5, 5)], p_core))
    g_core[0].wait()
    g_y1 = []
    for k in range(5):
        add_packed(gs2, k, go1, k, gr1, k)
        g_y1.append(send(gs2.at[k], gr2.at[k], p_y1))
    g_partials(go1, 5, 3)
    a_partials(as1, 0, 0)
    a_core = [send(as1.at[pl.ds(0, 8)], ar1.at[pl.ds(0, 8)], p_core)]
    a_partials(ao1, 0, 1)
    for i in range(2):
        load_w(i).start()
    g_core[1].wait()
    add_blocks(go1, 5, 5, go1, 5, gr1, 5)
    g_y2 = []
    for k in range(3):
        g_y1[k].wait()
        add_packed(gs3, k, go1, 5 + k, gr2, k)
        g_y2.append(send(gs3.at[k], gr3.at[k], p_y2))
    a_partials(as1, 8, 2)
    a_core.append(send(as1.at[pl.ds(8, 8)], ar1.at[pl.ds(8, 8)], p_core))
    a_core[0].wait()
    a_y1 = []

    def a_first(i):
        add_blocks(as2, 4 * i, 4, ao1, 4 * i, ar1, 4 * i)
        a_y1.append(send(as2.at[pl.ds(4 * i, 4)], ar2.at[pl.ds(4 * i, 4)], p_y1))

    a_partials(ao1, 8, 3)
    a_first(0)
    g_over = []
    for k in range(3):
        mine = (8, 9, 7)[k]
        g_y2[k].wait()
        if k < 2:
            g_y1[3 + k].wait()
        add_packed(go1, mine, go1, mine, gr2, mine - 5)
        add_packed(gs4, k, go1, mine, gr3, k)
        g_over.append((send(gs4.at[k], gx0.at[k], p_straight), send(gs4.at[k], gx1.at[k], p_cross)))
    a_first(1)
    a_core[1].wait()
    add_blocks(ao1, 8, 8, ao1, 8, ar1, 8)
    a_y1[0].wait()
    add_blocks(as3, 0, 4, ao1, 8, ar2, 0)
    a_y2 = [send(as3.at[pl.ds(2 * i, 2)], ar3.at[pl.ds(2 * i, 2)], p_y2) for i in range(2)]
    load_sweeps.wait()
    row, column = iotas(BLOCK, BLOCK)
    damp = jnp.where(row == column, DAMPING, 0.0).astype(F32)
    mean = 1.0 / tokens
    here, there = core * 10, o_core * 10
    g_own, g_r2, g_own_core, g_y3_core = [], [], [], []

    first = here + b1 * 5
    at = (first + b2 * 3, first + b2 * 3 + 1, first + 2)

    def g_invert(places):
        for k in places:
            for copy in g_over[k]:
                copy.wait()
        factors = [load_full_sum(gx0, k, gx1, k) * mean + damp for k in places]
        for k, inverse in zip(places, newton(factors, [sweeps[0, hidden_blocks + at[k]] for k in places])):
            store_packed(own, k, inverse)

    def gather_first(k):
        g_own.append(send(own.at[k], y3.at[k], p_y1))

    def gather_second(k):
        g_r2.append(send(own.at[k], r2.at[k], p_y2))

    def gather_core(k):
        g_own_core.append(send(own.at[k], d_own.at[k], p_core))

    relayed, y2_core = [], []

    def relay(k):
        g_r2[k].wait()
        relayed.append((send(r2.at[k], y2.at[k], p_y1), send(r2.at[k], d_r2.at[k], p_core)))

    def pass_own(k):
        g_own[k].wait()
        g_y3_core.append(send(y3.at[k], d_y3.at[k], p_core))

    def pass_y2(k):
        relayed[k][0].wait()
        y2_core.append(send(y2.at[k], d_y2.at[k], p_core))

    def apply(src, i, block):
        rows = pl.ds(pl.multiple_of(block * BLOCK, BLOCK), BLOCK)
        inverse = load_full(src, i).astype(BF16)
        applied[0, rows, :] = jnp.dot(inverse, w[rows, :], preferred_element_type=F32).astype(BF16)

    def apply_own(src, group, bit):
        for k in range(3):
            apply(src, k, group + (bit * 3 + k if k < 2 else 2))

    def apply_r2(src, group, bit):
        for k in range(2):
            apply(src, k, group + bit * 3 + k)

    g_invert((0, 1))
    gather_second(0)
    gather_second(1)
    gather_core(0)
    gather_core(1)
    a_y1[1].wait()
    add_blocks(ao1, 12, 4, ao1, 12, ar2, 4)
    a_y2[0].wait()
    add_blocks(as4, 0, 2, ao1, 12, ar3, 0)
    a_x = send(as4, ar4, p_x)
    a_y2[1].wait()
    add_blocks(ao1, 14, 2, ao1, 14, ar3, 2)
    gather_first(0)
    g_invert((2,))
    gather_core(2)
    gather_first(1)
    gather_first(2)
    for i in range(2):
        load_w(i).wait()
    apply_own(own, first, b2)
    relay(0)
    relay(1)
    apply_r2(r2, first, n2)
    for k in range(3):
        g_own_core[k].wait()
    apply_own(d_own, there + b2 * 5, b1)
    for k in range(3):
        pass_own(k)
    a_x.wait()
    factors = [load_full_sum(ao1, 14 + j, ar4, j) * mean + damp for j in range(2)]
    for j, inverse in enumerate(newton(factors, [sweeps[0, dp * 2 + j] for j in range(2)])):
        inv_a[j, :, :] = inverse.astype(BF16)
    pass_y2(0)
    apply_own(y3, here + n1 * 5, b2)
    pass_y2(1)
    apply_r2(y2, here + n1 * 5, n2)
    for k in range(2):
        relayed[k][1].wait()
    apply_r2(d_r2, there + b2 * 5, n1)
    for k in range(3):
        g_y3_core[k].wait()
    apply_own(d_y3, there + n2 * 5, b1)
    for k in range(2):
        y2_core[k].wait()
    apply_r2(d_y2, there + n2 * 5, n1)


def packed(count):
    return pltpu.VMEM((count, ROWS, HALF), BF16)


def exchange(tokens, sweeps, acts, grads, head, weights):
    hbm = pl.BlockSpec(memory_space=pltpu.HBM)
    vmem = pl.BlockSpec(memory_space=pltpu.VMEM)
    operands = [pltpu.with_memory_space_constraint(a, pltpu.HBM) for a in (sweeps, acts, grads, head, weights)]
    rows = acts.shape[1]
    g_counts = (10, 10, 10, 5, 5, 3, 3, 3, 3, 3)
    gather_counts = (3, 2, 3, 2, 3, 2, 3, 2)
    a_counts = (16, 16, 16, 8, 8, 4, 4, 2, 2)
    return pl.pallas_call(
        functools.partial(exchange_kernel, tokens),
        out_shape=(pltpu.VMEM(weights.shape, BF16), pltpu.VMEM((2, BLOCK, BLOCK), BF16)),
        in_specs=[hbm] * 5,
        out_specs=(vmem, vmem),
        scratch_shapes=[
            pltpu.SMEM(sweeps.shape, jnp.int32),
            pltpu.VMEM((rows, acts.shape[2]), BF16),
            pltpu.VMEM((rows, grads.shape[2]), BF16),
            pltpu.VMEM(weights.shape[1:], BF16),
            *[packed(n) for n in g_counts + gather_counts + a_counts],
            pltpu.SemaphoreType.DMA((23,)),
            pltpu.SemaphoreType.DMA((41,)),
            pltpu.SemaphoreType.DMA((41,)),
        ],
        compiler_params=pltpu.CompilerParams(
            collective_id=0, has_side_effects=True, vmem_limit_bytes=44 * 1024 * 1024
        ),
        name="exchange",
    )(*operands)


def finish_kernel(applied, inv_a, out, tiles, sems):
    rows = 2 * BLOCK
    copies = []
    for i in range(tiles.shape[0] // rows):
        part = pl.ds(i * rows, rows)
        for j in range(2):
            columns = slice(j * BLOCK, (j + 1) * BLOCK)
            tiles[part, columns] = jnp.dot(
                applied[0, part, columns], inv_a[j], preferred_element_type=F32
            ).astype(BF16)
        copies.append(pltpu.make_async_copy(tiles.at[part, :], out.at[0, part, :], sems.at[i]))
        copies[-1].start()
    for copy in copies:
        copy.wait()


def finish(applied, inv_a):
    vmem = pl.BlockSpec(memory_space=pltpu.VMEM)
    return pl.pallas_call(
        finish_kernel,
        out_shape=jax.ShapeDtypeStruct(applied.shape, applied.dtype),
        in_specs=[vmem, vmem],
        out_specs=pl.BlockSpec(memory_space=pltpu.HBM),
        scratch_shapes=[
            pltpu.VMEM(applied.shape[1:], applied.dtype),
            pltpu.SemaphoreType.DMA((applied.shape[1] // (2 * BLOCK),)),
        ],
        compiler_params=pltpu.CompilerParams(vmem_limit_bytes=12 * 1024 * 1024),
        name="finish",
    )(applied, inv_a)


def on_device(acts, input_grads, head_grads, weight_grad, sweeps):
    tokens = acts.shape[1] * lax.axis_size("dp")
    return finish(*exchange(tokens, sweeps, acts, input_grads, head_grads, weight_grad))


def solution(mesh):
    return jax.shard_map(
        on_device,
        mesh=mesh,
        in_specs=(
            P("section", "dp", None),
            P("section", "dp", None),
            P("dp", None),
            P("section", None, "dp"),
            P("section", None),
        ),
        out_specs=P("section", None, "dp"),
        check_vma=False,
    )
```

```python
import functools

import jax
import jax.numpy as jnp
from jax import lax
from jax.experimental import pallas as pl
from jax.experimental.pallas import tpu as pltpu
from jax.sharding import PartitionSpec as P

BLOCK = 256
HALF = 128
ROWS = 272
DAMPING = 0.05
F32 = jnp.float32
BF16 = jnp.bfloat16
MESH = pl.DeviceIdType.MESH


def iotas(rows, columns):
    return (
        lax.broadcasted_iota(jnp.int32, (rows, columns), 0),
        lax.broadcasted_iota(jnp.int32, (rows, columns), 1),
    )


def store_diagonals(dst, i, both):
    high = both.astype(BF16)
    low = both - high.astype(F32)
    dst[i, pl.ds(BLOCK, 16), :] = jnp.concatenate([high.astype(F32), low], axis=0).astype(BF16)


def store_packed(dst, i, full):
    row, column = iotas(HALF, HALF)
    first, off, last = full[:HALF, :HALF], full[:HALF, HALF:], full[HALF:, HALF:]
    dst[i, pl.ds(0, HALF), :] = jnp.where(row <= column, first, last).astype(BF16)
    dst[i, pl.ds(HALF, HALF), :] = off.astype(BF16)
    d_first = jnp.sum(jnp.where(row == column, first, 0.0), axis=0, keepdims=True)
    d_last = jnp.sum(jnp.where(row == column, last, 0.0), axis=0, keepdims=True)
    row8, _ = iotas(8, HALF)
    both = jnp.where(row8 == 0, d_first, jnp.where(row8 == 1, d_last, 0.0))
    store_diagonals(dst, i, both)


def add_packed(dst, di, a, ai, b, bi):
    dst[di, pl.ds(0, BLOCK), :] = (
        a[ai, pl.ds(0, BLOCK), :].astype(F32) + b[bi, pl.ds(0, BLOCK), :].astype(F32)
    ).astype(BF16)
    total = a[ai, pl.ds(BLOCK, 16), :].astype(F32) + b[bi, pl.ds(BLOCK, 16), :].astype(F32)
    store_diagonals(dst, di, total[:8] + total[8:])


def unpack(selected, off, both):
    row, column = iotas(HALF, HALF)
    flipped = selected.T
    first = jnp.where(row == column, both[0:1], jnp.where(row <= column, selected, flipped))
    last = jnp.where(row == column, both[1:2], jnp.where(row > column, selected, flipped))
    return jnp.concatenate(
        [jnp.concatenate([first, off], axis=1), jnp.concatenate([off.T, last], axis=1)], axis=0
    )


def load_full(src, i):
    tail = src[i, pl.ds(BLOCK, 16), :].astype(F32)
    return unpack(
        src[i, pl.ds(0, HALF), :].astype(F32),
        src[i, pl.ds(HALF, HALF), :].astype(F32),
        tail[:8] + tail[8:],
    )


def load_full_sum(a, ai, b, bi):
    both = [
        a[ai, pl.ds(start, size), :].astype(F32) + b[bi, pl.ds(start, size), :].astype(F32)
        for start, size in ((0, HALF), (HALF, HALF), (BLOCK, 16))
    ]
    return unpack(both[0], both[1], both[2][:8] + both[2][8:])


def split(x):
    high = x.astype(BF16)
    return high, (x - high.astype(F32)).astype(BF16)


def product(a, b):
    a_high, a_low = split(a)
    b_high, b_low = split(b)
    left = jnp.concatenate([a_high, a_high, a_low], axis=1)
    right = jnp.concatenate([b_high, b_low, b_high], axis=0)
    return jnp.dot(left, right, preferred_element_type=F32)


def newton(matrices, counts):
    row, column = iotas(BLOCK, BLOCK)
    eye = jnp.where(row == column, 1.0, 0.0).astype(F32)
    state = []
    for matrix in matrices:
        norm = jnp.max(jnp.sum(jnp.abs(matrix), axis=0, keepdims=True), axis=1, keepdims=True)
        scale = 1.0 / norm
        residual = eye - scale * matrix
        approx = scale * (eye + residual)
        state.append((approx, residual))
    chosen = [approx for approx, _ in state]
    state = [(approx, product(residual, residual)) for approx, residual in state]
    for turn in range(1, 4):
        if turn < 3:
            both = [product(jnp.concatenate([residual, approx], axis=0), residual) for approx, residual in state]
            state = [(approx + b[BLOCK:], b[:BLOCK]) for (approx, _), b in zip(state, both)]
        else:
            state = [(approx + product(approx, residual), None) for approx, residual in state]
        chosen = [jnp.where(count > turn, now, old) for count, (now, _), old in zip(counts, state, chosen)]
    return chosen


def exchange_kernel(
    tokens, sweeps_hbm, acts, grads, head, weights, applied, inv_a, sweeps,
    x_a, x_g, w, gs1, go1, gr1, gs2, gr2, gs3, gr3, gs4, gx0, gx1,
    own, r2, y3, y2, d_own, d_r2, d_y3, d_y2,
    as1, ao1, ar1, as2, ar2, as3, ar3, as4, ar4, load_sem, send_sem, recv_sem,
):
    section = lax.axis_index("section")
    dp = lax.axis_index("dp")
    core = lax.rem(dp, 2)
    y = lax.rem(dp // 2, 4)
    x = dp // 8
    y_low, y_high = lax.rem(y, 2), y // 2
    y_odd = lax.rem(y_low + y_high, 2)
    near = y + 1 - 2 * y_low
    far = 3 - y
    first_y = jnp.where(core == 0, near, far)
    second_y = jnp.where(core == 0, far, near)
    b1 = jnp.where(core == 0, y_odd, y_high)
    b2 = jnp.where(core == 0, y_high, y_odd)
    n1, n2 = 1 - b1, 1 - b2
    crossed = lax.rem(dp + 8, 16)
    below, above = lax.rem(section + 7, 8), lax.rem(section + 1, 8)
    p_core = (section, dp + 1 - 2 * core)
    p_y1 = (section, x * 8 + first_y * 2 + core)
    p_y2 = (section, x * 8 + second_y * 2 + core)
    p_x = (section, crossed)
    p_straight = (below, dp)
    p_cross = (below, crossed)
    used = []

    def send(src, dst, target):
        i = len(used)
        used.append(i)
        copy = pltpu.make_async_remote_copy(
            src_ref=src, dst_ref=dst, send_sem=send_sem.at[i], recv_sem=recv_sem.at[i],
            device_id=target, device_id_type=MESH,
        )
        copy.start()
        return copy

    w_chunk = w.shape[0] // 2
    hidden_blocks = x_a.shape[1] // BLOCK
    o_core = 1 - core
    g_groups = (o_core * 2 + n2, core * 2 + n1, o_core * 2 + b2, core * 2 + b1)
    a_groups = ((o_core, n2, b1), (core, n1, b2), (o_core, b2, b1), (core, b1, b2))

    def load_g(i, src):
        part = pl.ds(pl.multiple_of(g_groups[i] * 5 * BLOCK, BLOCK), 5 * BLOCK)
        return pltpu.make_async_copy(src.at[:, part], x_g.at[:, part], load_sem.at[i])

    def leaf(of_core, first, bit, u):
        middle = lax.rem(first + bit, 2)
        return (1 - x if u == 0 else x) * 8 + (jnp.where(of_core == 0, bit, first) * 2 + middle) * 2 + of_core

    def load_a(i, b, u):
        of_core, first, second = a_groups[i]
        owner = leaf(of_core, first, second if b else 1 - second, u)
        part = pl.ds(pl.multiple_of(owner * 2 * BLOCK, 2 * BLOCK), 2 * BLOCK)
        return pltpu.make_async_copy(acts.at[0, :, part], x_a.at[:, part], load_sem.at[4 + i * 4 + b * 2 + u])

    a_loads = [(b, u) for b in range(2) for u in range(2)]

    def load_w(i):
        part = pl.ds(i * w_chunk, w_chunk)
        return pltpu.make_async_copy(weights.at[0, part, :], w.at[part, :], load_sem.at[20 + i])

    @pl.when(section == 0)
    def _():
        for i in range(4):
            load_g(i, head).start()

    @pl.when(section > 0)
    def _():
        for i in range(4):
            load_g(i, grads.at[0]).start()

    load_sweeps = pltpu.make_async_copy(sweeps_hbm, sweeps, load_sem.at[22])
    load_sweeps.start()
    barrier = pltpu.get_barrier_semaphore()
    greeted = (p_core, p_y1, p_y2, p_x, p_straight, p_cross, (above, dp), (above, crossed))
    for target in greeted:
        pl.semaphore_signal(barrier, inc=1, device_id=target, device_id_type=MESH)

    def outer(ref, block):
        columns = pl.ds(pl.multiple_of(block * BLOCK, BLOCK), BLOCK)
        tile = ref[:, columns]
        return lax.dot_general(tile, tile, (((0,), (0,)), ((), ())), preferred_element_type=F32)

    def place(k, bit):
        return (1 - bit) * 3 + k if k < 2 else 2 if k == 2 else bit * 3 + k - 3

    def g_partials(dst, at, i):
        load_g(i, head).wait()
        bit = (b1, b2)[i % 2]
        for k in range(5):
            store_packed(dst, at + k, outer(x_g, g_groups[i] * 5 + place(k, bit)))

    def a_partials(dst, at, i):
        of_core, first, second = a_groups[i]
        for b, u in a_loads:
            load_a(i, b, u).wait()

        @pl.loop(0, 2)
        def _(e):
            bit = jnp.where(e == 0, 1 - second, second)
            for u in range(2):
                owner = leaf(of_core, first, bit, u)
                for j in range(2):
                    store_packed(dst, at + 4 * e + 2 * u + j, outer(x_a, owner * 2 + j))

    def add_blocks(dst, di, size, a, ai, b, bi):
        @pl.loop(0, size)
        def _(i):
            add_packed(dst, di + i, a, ai + i, b, bi + i)

    g_partials(gs1, 0, 0)
    for i in range(4):
        for b, u in a_loads:
            load_a(i, b, u).start()
    pl.semaphore_wait(barrier, len(greeted))
    g_core = [send(gs1.at[pl.ds(0, 5)], gr1.at[pl.ds(0, 5)], p_core)]
    g_partials(go1, 0, 1)
    g_partials(gs1, 5, 2)
    g_core.append(send(gs1.at[pl.ds(5, 5)], gr1.at[pl.ds(5, 5)], p_core))
    g_core[0].wait()
    g_y1 = []
    for k in range(5):
        add_packed(gs2, k, go1, k, gr1, k)
        g_y1.append(send(gs2.at[k], gr2.at[k], p_y1))
    g_partials(go1, 5, 3)
    a_partials(as1, 0, 0)
    a_core = [send(as1.at[pl.ds(0, 8)], ar1.at[pl.ds(0, 8)], p_core)]
    a_partials(ao1, 0, 1)
    for i in range(2):
        load_w(i).start()
    g_core[1].wait()
    add_blocks(go1, 5, 5, go1, 5, gr1, 5)
    g_y2 = []
    for k in range(3):
        g_y1[k].wait()
        add_packed(gs3, k, go1, 5 + k, gr2, k)
        g_y2.append(send(gs3.at[k], gr3.at[k], p_y2))
    a_partials(as1, 8, 2)
    a_core.append(send(as1.at[pl.ds(8, 8)], ar1.at[pl.ds(8, 8)], p_core))
    a_core[0].wait()
    a_y1 = []

    def a_first(i):
        add_blocks(as2, 4 * i, 4, ao1, 4 * i, ar1, 4 * i)
        a_y1.append(send(as2.at[pl.ds(4 * i, 4)], ar2.at[pl.ds(4 * i, 4)], p_y1))

    a_partials(ao1, 8, 3)
    a_first(0)
    g_over = []
    for k in range(3):
        mine = (8, 9, 7)[k]
        g_y2[k].wait()
        if k < 2:
            g_y1[3 + k].wait()
        add_packed(go1, mine, go1, mine, gr2, mine - 5)
        add_packed(gs4, k, go1, mine, gr3, k)
        g_over.append((send(gs4.at[k], gx0.at[k], p_straight), send(gs4.at[k], gx1.at[k], p_cross)))
    a_first(1)
    a_core[1].wait()
    add_blocks(ao1, 8, 8, ao1, 8, ar1, 8)
    a_y1[0].wait()
    add_blocks(as3, 0, 4, ao1, 8, ar2, 0)
    a_y2 = [send(as3.at[pl.ds(2 * i, 2)], ar3.at[pl.ds(2 * i, 2)], p_y2) for i in range(2)]
    load_sweeps.wait()
    row, column = iotas(BLOCK, BLOCK)
    damp = jnp.where(row == column, DAMPING, 0.0).astype(F32)
    mean = 1.0 / tokens
    here, there = core * 10, o_core * 10
    g_own, g_r2, g_own_core, g_y3_core = [], [], [], []

    first = here + b1 * 5
    at = (first + b2 * 3, first + b2 * 3 + 1, first + 2)

    def g_invert(places):
        for k in places:
            for copy in g_over[k]:
                copy.wait()
        factors = [load_full_sum(gx0, k, gx1, k) * mean + damp for k in places]
        for k, inverse in zip(places, newton(factors, [sweeps[0, hidden_blocks + at[k]] for k in places])):
            store_packed(own, k, inverse)

    def gather_first(k):
        g_own.append(send(own.at[k], y3.at[k], p_y1))

    def gather_second(k):
        g_r2.append(send(own.at[k], r2.at[k], p_y2))

    def gather_core(k):
        g_own_core.append(send(own.at[k], d_own.at[k], p_core))

    relayed, y2_core = [], []

    def relay(k):
        g_r2[k].wait()
        relayed.append((send(r2.at[k], y2.at[k], p_y1), send(r2.at[k], d_r2.at[k], p_core)))

    def pass_own(k):
        g_own[k].wait()
        g_y3_core.append(send(y3.at[k], d_y3.at[k], p_core))

    def pass_y2(k):
        relayed[k][0].wait()
        y2_core.append(send(y2.at[k], d_y2.at[k], p_core))

    def apply(src, i, block):
        rows = pl.ds(pl.multiple_of(block * BLOCK, BLOCK), BLOCK)
        inverse = load_full(src, i).astype(BF16)
        applied[0, rows, :] = jnp.dot(inverse, w[rows, :], preferred_element_type=F32).astype(BF16)

    def apply_own(src, group, bit):
        for k in range(3):
            apply(src, k, group + (bit * 3 + k if k < 2 else 2))

    def apply_r2(src, group, bit):
        for k in range(2):
            apply(src, k, group + bit * 3 + k)

    g_invert((0, 1))
    gather_second(0)
    gather_second(1)
    gather_core(0)
    gather_core(1)
    a_y1[1].wait()
    add_blocks(ao1, 12, 4, ao1, 12, ar2, 4)
    a_y2[0].wait()
    add_blocks(as4, 0, 2, ao1, 12, ar3, 0)
    a_x = send(as4, ar4, p_x)
    gather_first(0)
    g_invert((2,))
    gather_core(2)
    gather_first(1)
    gather_first(2)
    a_y2[1].wait()
    add_blocks(ao1, 14, 2, ao1, 14, ar3, 2)
    for i in range(2):
        load_w(i).wait()
    relay(0)
    relay(1)
    apply_own(own, first, b2)
    apply_r2(r2, first, n2)
    for k in range(3):
        g_own_core[k].wait()
    apply_own(d_own, there + b2 * 5, b1)
    for k in range(3):
        pass_own(k)
    a_x.wait()
    factors = [load_full_sum(ao1, 14 + j, ar4, j) * mean + damp for j in range(2)]
    for j, inverse in enumerate(newton(factors, [sweeps[0, dp * 2 + j] for j in range(2)])):
        inv_a[j, :, :] = inverse.astype(BF16)
    pass_y2(0)
    apply_own(y3, here + n1 * 5, b2)
    pass_y2(1)
    apply_r2(y2, here + n1 * 5, n2)
    for k in range(2):
        relayed[k][1].wait()
    apply_r2(d_r2, there + b2 * 5, n1)
    for k in range(3):
        g_y3_core[k].wait()
    apply_own(d_y3, there + n2 * 5, b1)
    for k in range(2):
        y2_core[k].wait()
    apply_r2(d_y2, there + n2 * 5, n1)


def packed(count):
    return pltpu.VMEM((count, ROWS, HALF), BF16)


def exchange(tokens, sweeps, acts, grads, head, weights):
    hbm = pl.BlockSpec(memory_space=pltpu.HBM)
    vmem = pl.BlockSpec(memory_space=pltpu.VMEM)
    operands = [pltpu.with_memory_space_constraint(a, pltpu.HBM) for a in (sweeps, acts, grads, head, weights)]
    rows = acts.shape[1]
    g_counts = (10, 10, 10, 5, 5, 3, 3, 3, 3, 3)
    gather_counts = (3, 2, 3, 2, 3, 2, 3, 2)
    a_counts = (16, 16, 16, 8, 8, 4, 4, 2, 2)
    return pl.pallas_call(
        functools.partial(exchange_kernel, tokens),
        out_shape=(pltpu.VMEM(weights.shape, BF16), pltpu.VMEM((2, BLOCK, BLOCK), BF16)),
        in_specs=[hbm] * 5,
        out_specs=(vmem, vmem),
        scratch_shapes=[
            pltpu.SMEM(sweeps.shape, jnp.int32),
            pltpu.VMEM((rows, acts.shape[2]), BF16),
            pltpu.VMEM((rows, grads.shape[2]), BF16),
            pltpu.VMEM(weights.shape[1:], BF16),
            *[packed(n) for n in g_counts + gather_counts + a_counts],
            pltpu.SemaphoreType.DMA((23,)),
            pltpu.SemaphoreType.DMA((41,)),
            pltpu.SemaphoreType.DMA((41,)),
        ],
        compiler_params=pltpu.CompilerParams(
            collective_id=0, has_side_effects=True, vmem_limit_bytes=44 * 1024 * 1024
        ),
        name="exchange",
    )(*operands)


def finish_kernel(applied, inv_a, out, tiles, sems):
    rows = 2 * BLOCK
    copies = []
    for i in range(tiles.shape[0] // rows):
        part = pl.ds(i * rows, rows)
        for j in range(2):
            columns = slice(j * BLOCK, (j + 1) * BLOCK)
            tiles[part, columns] = jnp.dot(
                applied[0, part, columns], inv_a[j], preferred_element_type=F32
            ).astype(BF16)
        copies.append(pltpu.make_async_copy(tiles.at[part, :], out.at[0, part, :], sems.at[i]))
        copies[-1].start()
    for copy in copies:
        copy.wait()


def finish(applied, inv_a):
    vmem = pl.BlockSpec(memory_space=pltpu.VMEM)
    return pl.pallas_call(
        finish_kernel,
        out_shape=jax.ShapeDtypeStruct(applied.shape, applied.dtype),
        in_specs=[vmem, vmem],
        out_specs=pl.BlockSpec(memory_space=pltpu.HBM),
        scratch_shapes=[
            pltpu.VMEM(applied.shape[1:], applied.dtype),
            pltpu.SemaphoreType.DMA((applied.shape[1] // (2 * BLOCK),)),
        ],
        compiler_params=pltpu.CompilerParams(vmem_limit_bytes=12 * 1024 * 1024),
        name="finish",
    )(applied, inv_a)


def on_device(acts, input_grads, head_grads, weight_grad, sweeps):
    tokens = acts.shape[1] * lax.axis_size("dp")
    return finish(*exchange(tokens, sweeps, acts, input_grads, head_grads, weight_grad))


def solution(mesh):
    return jax.shard_map(
        on_device,
        mesh=mesh,
        in_specs=(
            P("section", "dp", None),
            P("section", "dp", None),
            P("dp", None),
            P("section", None, "dp"),
            P("section", None),
        ),
        out_specs=P("section", None, "dp"),
        check_vma=False,
    )
```
